32 devices in a mesh: panels: 32 (over z, y, x, core).
Axes of the slice: x: 2, y: 2, z: 4, core: 2. Of those that a mesh axis runs over, the one named last changes fastest.
Arguments:
- excitation: bfloat16 [64, 131072], P(None, 'panels'), may hold values from -6 to 6
- near_tiles: bfloat16 [512, 5, 256, 256], P('panels'), may hold values from -0.15625 to 0.15625
- near_offset: int32 [512, 5], P('panels'), may hold values from -16 to 16, as said below
- near_count: int32 [512], P('panels'), may hold values from 1 to 5, as said below
- far_src: int32 [32, 16], replicated, may hold values from 0 to 31, as said below
- far_count: int32 [32], replicated, may hold values from 1 to 16
- source_factor: bfloat16 [16, 32, 131072], P(None, None, 'panels'), may hold values from -0.09375 to 0.09375
- target_factor: bfloat16 [16, 32, 131072], P(None, None, 'panels'), may hold values from -0.25 to 0.25
Outputs:
- krylov: float32 [5, 64, 131072], P(None, None, 'panels')
The draws below stay inside these ranges and needn't reach their ends.
Inputs may be any that keep to these rules, and one draw needn't show every extreme that they name: `near_offset`: offsets within one leaf are distinct. `near_count`: some leaf has 5 live slots. `far_src`: within a row the entries are distinct and never the row itself. Counting live slots only, every block row is the source of at most 16 far blocks, and some block row of exactly 16.
All inputs are finite; a program needn't handle non-finite values.
Results may differ from the reference program's by a relative error of at most 0.0095.
Values may be sent and summed in bfloat16 or wider, within the bound.
A program may use at most 128 MiB of HBM per device.

```python
import jax
import jax.numpy as jnp
from jax import lax

LEAF = 256
EXCITE = 64
RANK = 32
NEAR = 5
FAR = 16
ITERS = 5
LEAVES_DEV = 16
PANELS_DEV = 4096
LEAVES = 512
PANELS = 131072
DEVS = 32


def draw_near_offset(key, part):
    choices_total = 2 * LEAVES_DEV + 1
    scores = jax.random.randint(key, (LEAVES, choices_total), 0, 1 << 20) * 128
    scores = scores + jnp.arange(choices_total, dtype=jnp.int32)[None, :]
    order = jnp.argsort(scores, axis=1)
    return (order[:, :NEAR] - LEAVES_DEV).astype(jnp.int32)


def draw_near_count(key, part):
    first_key, second_key = jax.random.split(key)
    counts = jax.random.randint(first_key, (LEAVES,), 1, NEAR + 1)
    pivot = jax.random.randint(second_key, (), 0, LEAVES)
    return counts.at[pivot].set(NEAR).astype(jnp.int32)


def far_plan(key):
    base = jax.random.fold_in(key, 7)
    perm_key, offset_key, slot_key, pivot_key = jax.random.split(base, 4)
    order = jax.random.permutation(perm_key, DEVS).astype(jnp.int32)
    inverse = jnp.zeros((DEVS,), jnp.int32).at[order].set(jnp.arange(DEVS, dtype=jnp.int32))
    offset_scores = jax.random.randint(offset_key, (DEVS - 1,), 0, 1 << 16) * DEVS
    offset_scores = offset_scores + jnp.arange(DEVS - 1, dtype=jnp.int32)
    offsets = (jnp.argsort(offset_scores)[:FAR] + 1).astype(jnp.int32)
    slot_scores = jax.random.randint(slot_key, (DEVS, FAR), 0, 1 << 16) * FAR
    slot_scores = slot_scores + jnp.arange(FAR, dtype=jnp.int32)[None, :]
    slot_order = jnp.argsort(slot_scores, axis=1).astype(jnp.int32)
    shifts = jnp.take(offsets, slot_order)
    far_src = jnp.take(inverse, (order[:, None] + shifts) % DEVS)
    pivot = jax.random.randint(pivot_key, (), 0, DEVS)
    full_rows = jnp.take(inverse, (order[pivot] - offsets) % DEVS)
    return (far_src.astype(jnp.int32), full_rows.astype(jnp.int32))


def draw_far_src(key, part):
    far_src, full_rows = far_plan(key)
    return far_src


def draw_far_count(key, part):
    far_src, full_rows = far_plan(key)
    own = jax.random.fold_in(key, 11)
    first_key, second_key = jax.random.split(own)
    left = jax.random.randint(first_key, (DEVS,), 0, FAR + 1)
    right = jax.random.randint(second_key, (DEVS,), 0, FAR + 1)
    counts = jnp.clip(1 + left * right // FAR, 1, FAR)
    return counts.at[full_rows].set(FAR).astype(jnp.int32)


def level_of(own_key, dims, pieces, low, high):
    factor_of, own = 1.0, jax.random.fold_in(own_key, 6)
    for axis_at, blocks in pieces:
        heights = jnp.exp(jax.random.uniform(jax.random.fold_in(own, axis_at), (blocks,), jnp.float32, low / len(pieces), high / len(pieces)))
        factor_of = factor_of * jnp.repeat(heights, dims[axis_at] // blocks).reshape([-1 if axis == axis_at else 1 for axis in range(len(dims))])
    return factor_of


def bell_draw(rng, dims, width, bound, shards=(), kind=jnp.bfloat16):
    values = width * jax.random.normal(rng, dims, jnp.float32)
    if shards:
        values = values * level_of(rng, dims, shards, -0.22, 0.18)
    return jnp.clip(values, -bound, bound).astype(kind)


def setup_inputs(seed: int = 0) -> dict:
    splits = jax.random.split(jax.random.key(seed), 9)
    excitation = bell_draw(splits[0], (EXCITE, PANELS), 1.0, 6.0, ((1, 32),))
    near_tiles = bell_draw(splits[1], (LEAVES, NEAR, LEAF, LEAF), (NEAR * LEAF) ** -0.5, 0.15625, ((0, 32),))
    near_offset = draw_near_offset(jax.random.fold_in(splits[8], 71), 0)
    near_count = draw_near_count(jax.random.fold_in(splits[8], 71), 0)
    far_src = draw_far_src(jax.random.fold_in(splits[8], 71), 0)
    far_count = draw_far_count(jax.random.fold_in(splits[8], 71), 0)
    source_factor = bell_draw(splits[6], (FAR, RANK, PANELS), PANELS_DEV ** -0.5, 0.09375, ((2, 32),))
    target_factor = bell_draw(splits[7], (FAR, RANK, PANELS), (RANK * FAR) ** -0.5, 0.25, ((2, 32),))
    return dict(excitation=excitation, near_tiles=near_tiles, near_offset=near_offset, near_count=near_count, far_src=far_src, far_count=far_count, source_factor=source_factor, target_factor=target_factor)


def out_ranks(far_src, far_count):
    row_total, slot_count = far_src.shape
    live_far = jnp.arange(slot_count, dtype=jnp.int32)[None, :] < far_count[:, None]
    owners = jnp.arange(row_total, dtype=jnp.int32)
    hits = ((far_src.reshape(-1)[:, None] == owners[None, :]) & live_far.reshape(-1)[:, None]).astype(jnp.int32)
    earlier = jnp.cumsum(hits, axis=0) - hits
    out_rank = jnp.sum(earlier * hits, axis=1).astype(jnp.int32)
    return out_rank.reshape(row_total, slot_count), live_far


def apply_operator(field, near_tiles, near_offset, near_count, far_src, out_rank, live_far, source_factor, target_factor):
    row_total = far_src.shape[0]
    leaf_total = near_tiles.shape[0]
    near_slots = near_tiles.shape[1]
    leaf_size = near_tiles.shape[2]
    leaves_local = leaf_total // row_total
    panels_local = leaves_local * leaf_size
    excite = field.shape[0]
    highest = lax.Precision.HIGHEST

    def coefficients(device):
        first = device * panels_local
        factor = lax.dynamic_slice_in_dim(source_factor, first, panels_local, 2).astype(jnp.float32)
        charges = lax.dynamic_slice_in_dim(field, first, panels_local, 1).astype(jnp.float32)
        return jnp.einsum('jrp,mp->jrm', factor, charges, precision=highest).astype(jnp.bfloat16)

    table = lax.map(coefficients, jnp.arange(row_total, dtype=jnp.int32))
    leaves = field.reshape(excite, leaf_total, leaf_size)

    def block_row(device):
        first_leaf = device * leaves_local
        tiles = lax.dynamic_slice_in_dim(near_tiles, first_leaf, leaves_local, 0).astype(jnp.float32)
        offsets = lax.dynamic_slice_in_dim(near_offset, first_leaf, leaves_local, 0)
        counts = lax.dynamic_slice_in_dim(near_count, first_leaf, leaves_local, 0)
        source_leaf = (first_leaf + jnp.arange(leaves_local, dtype=jnp.int32)[:, None] + offsets) % leaf_total
        picked = jnp.take(leaves, source_leaf.reshape(-1).astype(jnp.int32), axis=1)
        picked = picked.reshape(excite, leaves_local, near_slots, leaf_size).astype(jnp.float32)
        live_near = jnp.arange(near_slots, dtype=jnp.int32)[None, :] < counts[:, None]
        picked = jnp.where(live_near[None, :, :, None], picked, jnp.zeros_like(picked))
        near_part = jnp.einsum('ijab,mijb->mia', tiles, picked, precision=highest).reshape(excite, panels_local)
        sources = far_src[device]
        ranks = out_rank[device]
        live_slot = live_far[device]
        coef = table[sources, ranks].astype(jnp.float32)
        coef = jnp.where(live_slot[:, None, None], coef, jnp.zeros_like(coef))
        factor = lax.dynamic_slice_in_dim(target_factor, device * panels_local, panels_local, 2).astype(jnp.float32)
        far_part = jnp.einsum('jrm,jrp->mp', coef, factor, precision=highest)
        return near_part + far_part

    rows_out = lax.map(block_row, jnp.arange(row_total, dtype=jnp.int32))
    return jnp.transpose(rows_out, (1, 0, 2)).reshape(excite, row_total * panels_local)


def reference(excitation, near_tiles, near_offset, near_count, far_src, far_count, source_factor, target_factor):
    out_rank, live_far = out_ranks(far_src, far_count)
    current = excitation
    results = []
    for step in range(ITERS):
        result = apply_operator(current, near_tiles, near_offset, near_count, far_src, out_rank, live_far, source_factor, target_factor)
        results.append(result)
        current = result.astype(jnp.bfloat16)
    return jnp.stack(results, axis=0)
```

```python
import functools

import jax
import jax.numpy as jnp
from jax import lax
from jax.experimental import pallas as pl
from jax.experimental.pallas import tpu as pltpu
from jax.sharding import PartitionSpec as P

ITERS = 5
MESH = pl.DeviceIdType.MESH
NT = (((1,), (1,)), ((), ()))


def kernel(
    n,
    idx_ref,
    field_hbm,
    leaves_hbm,
    near_hbm,
    src_hbm,
    tgt_hbm,
    out_hbm,
    near,
    src,
    tgt,
    field,
    ext_a,
    ext_b,
    recv_a,
    recv_b,
    outg_a,
    outg_b,
    cbuf,
    gin,
    stage_a,
    stage_b,
    load_sem,
    out_sem,
    halo_send,
    halo_recv,
    far_send,
    far_recv,
):
    me = lax.axis_index("panels")
    right, left = lax.rem(me + 1, n), lax.rem(me + n - 1, n)
    leaves, excite, leaf = leaves_hbm.shape
    slots = near_hbm.shape[0] // leaves
    far_slots, rank, _ = cbuf.shape
    far_slots -= 1
    panels = leaves * leaf
    groups = 4 if leaves % 4 == 0 else 1
    size = leaves // groups
    exts, recvs, outgs, stages = (ext_a, ext_b), (recv_a, recv_b), (outg_a, outg_b), (stage_a, stage_b)

    loads = [
        pltpu.make_async_copy(field_hbm, field, load_sem.at[0]),
        pltpu.make_async_copy(leaves_hbm, ext_a.at[pl.ds(leaves, leaves)], load_sem.at[1]),
        pltpu.make_async_copy(src_hbm, src, load_sem.at[2]),
        pltpu.make_async_copy(tgt_hbm, tgt, load_sem.at[3]),
        pltpu.make_async_copy(near_hbm, near, load_sem.at[4]),
    ]
    for load in loads:
        load.start()

    for ext in exts:
        ext[3 * leaves] = jnp.zeros((excite, leaf), jnp.bfloat16)
    for recv in recvs:
        recv[n] = jnp.zeros((rank, excite), jnp.bfloat16)
        recv[me] = jnp.zeros((rank, excite), jnp.bfloat16)
    cbuf[far_slots] = jnp.zeros((rank, excite), jnp.bfloat16)

    barrier = pltpu.get_barrier_semaphore()

    @pl.loop(1, n)
    def _(d):
        pl.semaphore_signal(barrier, inc=1, device_id=(lax.rem(me + d, n),), device_id_type=MESH)

    pl.semaphore_wait(barrier, n - 1)

    def halo(k, g, side):
        ext = exts[k % 2]
        base = 0 if side == 0 else 2 * leaves
        return pltpu.make_async_remote_copy(
            src_ref=ext.at[pl.ds(leaves + g * size, size)],
            dst_ref=ext.at[pl.ds(base + g * size, size)],
            send_sem=halo_send.at[k % 2, side, g],
            recv_sem=halo_recv.at[k % 2, side, g],
            device_id=(right if side == 0 else left,),
            device_id_type=MESH,
        )

    def block(k, d):
        peer = lax.rem(me + d, n)
        return pltpu.make_async_remote_copy(
            src_ref=outgs[k % 2].at[peer],
            dst_ref=recvs[k % 2].at[me],
            send_sem=far_send.at[k % 2, d],
            recv_sem=far_recv.at[k % 2, d],
            device_id=(peer,),
            device_id_type=MESH,
        )

    loads[1].wait()
    for g in range(groups):
        halo(0, g, 0).start()
        halo(0, g, 1).start()
    loads[0].wait()
    loads[2].wait()

    half = src.shape[0] // 2
    rows_half = half // rank
    for k in range(ITERS):
        ext, recv, outg, stage = exts[k % 2], recvs[k % 2], outgs[k % 2], stages[k % 2]

        @pl.loop(0, 2)
        def _(h):
            part = lax.dot_general(
                src[pl.ds(pl.multiple_of(h * half, half), half), :],
                field[...],
                NT,
                preferred_element_type=jnp.float32,
            )
            cbuf[pl.ds(h * rows_half, rows_half)] = part.astype(jnp.bfloat16).reshape(rows_half, rank, excite)

        @pl.loop(0, n)
        def _(t):
            outg[t] = cbuf[idx_ref[leaves * slots + t]]

        @pl.loop(1, n)
        def _(d):
            block(k, d).start()

        if k >= 2:
            pltpu.make_async_copy(stage, out_hbm.at[k - 2], out_sem.at[k % 2]).wait()

        @pl.loop(1, n)
        def _(d):
            block(k, d).wait()

        for j in range(far_slots):
            gin[pl.ds(j * rank, rank), :] = recv[idx_ref[leaves * slots + n + j]].astype(jnp.float32)
        coef = gin[...].T.astype(jnp.bfloat16)
        if k == 0:
            loads[3].wait()

        @pl.loop(0, groups)
        def _(g):
            cols = pl.ds(pl.multiple_of(g * size * leaf, size * leaf), size * leaf)
            stage[:, cols] = jnp.dot(coef, tgt[:, cols], preferred_element_type=jnp.float32)

        if k == 0:
            loads[4].wait()
        for g in range(groups):
            halo(k, g, 0).wait()
            halo(k, g, 1).wait()

        @pl.loop(0, groups)
        def _(g):
            for u in range(size):
                i = g * size + u
                cols = pl.ds(pl.multiple_of(i * leaf, leaf), leaf)
                total = stage[:, cols]
                for j in range(slots):
                    total += lax.dot_general(
                        ext[idx_ref[i * slots + j]],
                        near[i * slots + j],
                        NT,
                        preferred_element_type=jnp.float32,
                    )
                stage[:, cols] = total
                if k < ITERS - 1:
                    rounded = total.astype(jnp.bfloat16)
                    field[:, cols] = rounded
                    exts[(k + 1) % 2][leaves + i] = rounded
            if k < ITERS - 1:

                @pl.when(g > 0)
                def _():
                    halo(k + 1, g - 1, 0).start()
                    halo(k + 1, g - 1, 1).start()

        if k < ITERS - 1:
            halo(k + 1, groups - 1, 0).start()
            halo(k + 1, groups - 1, 1).start()
        pltpu.make_async_copy(stage, out_hbm.at[k], out_sem.at[k % 2]).start()
    for k in range(max(ITERS - 2, 0), ITERS):
        pltpu.make_async_copy(stages[k % 2], out_hbm.at[k], out_sem.at[k % 2]).wait()


def shards(n, excitation, near_tiles, near_offset, near_count, far_src, far_count, source_factor, target_factor):
    excite, panels = excitation.shape
    leaves, slots, leaf, _ = near_tiles.shape
    far_slots, rank, _ = source_factor.shape
    me = lax.axis_index("panels")
    ints = jnp.int32

    own = jnp.arange(leaves, dtype=ints)[:, None] + leaves + near_offset
    near_idx = jnp.where(jnp.arange(slots, dtype=ints)[None, :] < near_count[:, None], own, 3 * leaves)
    live = jnp.arange(far_slots, dtype=ints)[None, :] < far_count[:, None]
    has = jnp.sum(((far_src == me) & live).astype(ints), axis=1)
    rows = jnp.arange(n, dtype=ints)
    before = jnp.sum(jnp.where(rows[None, :] < rows[:, None], has[None, :], 0), axis=1)
    send_idx = jnp.where(has > 0, before, far_slots)
    my_src = lax.dynamic_index_in_dim(far_src, me, 0, keepdims=False)
    my_live = lax.dynamic_index_in_dim(live, me, 0, keepdims=False)
    recv_idx = jnp.where(my_live, my_src, n)
    idx = jnp.concatenate([near_idx.reshape(-1), send_idx, recv_idx]).astype(ints)
    leaf_field = excitation.reshape(excite, leaves, leaf).transpose(1, 0, 2)

    bf, f32 = jnp.bfloat16, jnp.float32
    groups = 4 if leaves % 4 == 0 else 1
    hbm = pl.BlockSpec(memory_space=pl.ANY)
    return pl.pallas_call(
        functools.partial(kernel, n),
        out_shape=jax.ShapeDtypeStruct((ITERS, excite, panels), f32),
        in_specs=[pl.BlockSpec(memory_space=pltpu.SMEM)] + [hbm] * 5,
        out_specs=hbm,
        scratch_shapes=[
            pltpu.VMEM((leaves * slots, leaf, leaf), bf),
            pltpu.VMEM((far_slots * rank, panels), bf),
            pltpu.VMEM((far_slots * rank, panels), bf),
            pltpu.VMEM((excite, panels), bf),
            pltpu.VMEM((3 * leaves + 1, excite, leaf), bf),
            pltpu.VMEM((3 * leaves + 1, excite, leaf), bf),
            pltpu.VMEM((n + 1, rank, excite), bf),
            pltpu.VMEM((n + 1, rank, excite), bf),
            pltpu.VMEM((n, rank, excite), bf),
            pltpu.VMEM((n, rank, excite), bf),
            pltpu.VMEM((far_slots + 1, rank, excite), bf),
            pltpu.VMEM((far_slots * rank, excite), f32),
            pltpu.VMEM((excite, panels), f32),
            pltpu.VMEM((excite, panels), f32),
            pltpu.SemaphoreType.DMA((5,)),
            pltpu.SemaphoreType.DMA((2,)),
            pltpu.SemaphoreType.DMA((2, 2, groups)),
            pltpu.SemaphoreType.DMA((2, 2, groups)),
            pltpu.SemaphoreType.DMA((2, n)),
            pltpu.SemaphoreType.DMA((2, n)),
        ],
        compiler_params=pltpu.CompilerParams(
            collective_id=0, has_side_effects=True, vmem_limit_bytes=60 * 1024 * 1024
        ),
    )(
        idx,
        excitation,
        leaf_field,
        near_tiles.reshape(leaves * slots, leaf, leaf),
        source_factor.reshape(far_slots * rank, panels),
        target_factor.reshape(far_slots * rank, panels),
    )


def solution(mesh):
    in_specs = (
        P(None, "panels"),
        P("panels", None, None, None),
        P("panels", None),
        P("panels"),
        P(),
        P(),
        P(None, None, "panels"),
        P(None, None, "panels"),
    )
    return jax.shard_map(
        functools.partial(shards, mesh.shape["panels"]),
        mesh=mesh,
        in_specs=in_specs,
        out_specs=P(None, None, "panels"),
        check_vma=False,
    )
```

```python
import functools

import jax
import jax.numpy as jnp
from jax import lax
from jax.experimental import pallas as pl
from jax.experimental.pallas import tpu as pltpu
from jax.sharding import PartitionSpec as P

ITERS = 5
MESH = pl.DeviceIdType.MESH
NT = (((1,), (1,)), ((), ()))


def kernel(
    n,
    idx_ref,
    field_hbm,
    leaves_hbm,
    near_hbm,
    src_hbm,
    tgt_hbm,
    out_hbm,
    near,
    src,
    tgt,
    field,
    ext_a,
    ext_b,
    recv_a,
    recv_b,
    outg_a,
    outg_b,
    cbuf,
    gin,
    stage_a,
    stage_b,
    load_sem,
    out_sem,
    halo_send,
    halo_recv,
    far_send,
    far_recv,
):
    me = lax.axis_index("panels")
    right, left = lax.rem(me + 1, n), lax.rem(me + n - 1, n)
    leaves, excite, leaf = leaves_hbm.shape
    slots = near_hbm.shape[0] // leaves
    far_slots, pack, _ = cbuf.shape
    far_slots -= 1
    rank = src.shape[0] // far_slots
    panels = leaves * leaf
    groups = 4 if leaves % 4 == 0 else 1
    size = leaves // groups
    exts, recvs, outgs, stages = (ext_a, ext_b), (recv_a, recv_b), (outg_a, outg_b), (stage_a, stage_b)

    loads = [
        pltpu.make_async_copy(field_hbm, field, load_sem.at[0]),
        pltpu.make_async_copy(leaves_hbm, ext_a.at[pl.ds(leaves, leaves)], load_sem.at[1]),
        pltpu.make_async_copy(src_hbm, src, load_sem.at[2]),
        pltpu.make_async_copy(tgt_hbm, tgt, load_sem.at[3]),
        pltpu.make_async_copy(near_hbm, near, load_sem.at[4]),
    ]
    for load in loads:
        load.start()

    for ext in exts:
        ext[3 * leaves] = jnp.zeros((excite, leaf), jnp.bfloat16)
    for recv in recvs:
        recv[n] = jnp.zeros((pack, 2 * excite), jnp.bfloat16)
        recv[me] = jnp.zeros((pack, 2 * excite), jnp.bfloat16)
    cbuf[far_slots] = jnp.zeros((pack, 2 * excite), jnp.bfloat16)

    barrier = pltpu.get_barrier_semaphore()

    @pl.loop(1, n)
    def _(d):
        pl.semaphore_signal(barrier, inc=1, device_id=(lax.rem(me + d, n),), device_id_type=MESH)

    pl.semaphore_wait(barrier, n - 1)

    def halo(k, g, side):
        ext = exts[k % 2]
        base = 0 if side == 0 else 2 * leaves
        return pltpu.make_async_remote_copy(
            src_ref=ext.at[pl.ds(leaves + g * size, size)],
            dst_ref=ext.at[pl.ds(base + g * size, size)],
            send_sem=halo_send.at[k % 2, side, g],
            recv_sem=halo_recv.at[k % 2, side, g],
            device_id=(right if side == 0 else left,),
            device_id_type=MESH,
        )

    def block(k, d):
        peer = lax.rem(me + d, n)
        return pltpu.make_async_remote_copy(
            src_ref=outgs[k % 2].at[peer],
            dst_ref=recvs[k % 2].at[me],
            send_sem=far_send.at[k % 2, d],
            recv_sem=far_recv.at[k % 2, d],
            device_id=(peer,),
            device_id_type=MESH,
        )

    loads[1].wait()
    for g in range(groups):
        halo(0, g, 0).start()
        halo(0, g, 1).start()
    loads[0].wait()
    loads[2].wait()

    half = src.shape[0] // 2
    rows_half = half // rank
    for k in range(ITERS):
        ext, recv, outg, stage = exts[k % 2], recvs[k % 2], outgs[k % 2], stages[k % 2]

        @pl.loop(0, 2)
        def _(h):
            part = lax.dot_general(
                src[pl.ds(pl.multiple_of(h * half, half), half), :],
                field[...],
                NT,
                preferred_element_type=jnp.float32,
            )
            part = part.reshape(rows_half, 2, pack, excite)
            part = jnp.concatenate([part[:, 0], part[:, 1]], axis=2)
            cbuf[pl.ds(h * rows_half, rows_half)] = part.astype(jnp.bfloat16)

        @pl.loop(0, n)
        def _(t):
            outg[t] = cbuf[idx_ref[leaves * slots + t]]

        @pl.loop(1, n)
        def _(d):
            block(k, d).start()

        if k >= 2:
            pltpu.make_async_copy(stage, out_hbm.at[k - 2], out_sem.at[k % 2]).wait()

        @pl.loop(1, n)
        def _(d):
            block(k, d).wait()

        for j in range(far_slots):
            got = recv[idx_ref[leaves * slots + n + j]].astype(jnp.float32)
            gin[pl.ds(j * rank, pack), :] = got[:, :excite]
            gin[pl.ds(j * rank + pack, pack), :] = got[:, excite:]
        coef = gin[...].T.astype(jnp.bfloat16)
        if k == 0:
            loads[3].wait()

        @pl.loop(0, groups)
        def _(g):
            cols = pl.ds(pl.multiple_of(g * size * leaf, size * leaf), size * leaf)
            stage[:, cols] = jnp.dot(coef, tgt[:, cols], preferred_element_type=jnp.float32)

        if k == 0:
            loads[4].wait()
        for g in range(groups):
            halo(k, g, 0).wait()
            halo(k, g, 1).wait()

        @pl.loop(0, groups)
        def _(g):
            for u in range(size):
                i = g * size + u
                cols = pl.ds(pl.multiple_of(i * leaf, leaf), leaf)
                total = stage[:, cols]
                for j in range(slots):
                    total += lax.dot_general(
                        ext[idx_ref[i * slots + j]],
                        near[i * slots + j],
                        NT,
                        preferred_element_type=jnp.float32,
                    )
                stage[:, cols] = total
                if k < ITERS - 1:
                    rounded = total.astype(jnp.bfloat16)
                    field[:, cols] = rounded
                    exts[(k + 1) % 2][leaves + i] = rounded
            if k < ITERS - 1:

                @pl.when(g > 0)
                def _():
                    halo(k + 1, g - 1, 0).start()
                    halo(k + 1, g - 1, 1).start()

        if k < ITERS - 1:
            halo(k + 1, groups - 1, 0).start()
            halo(k + 1, groups - 1, 1).start()
        pltpu.make_async_copy(stage, out_hbm.at[k], out_sem.at[k % 2]).start()
    for k in range(max(ITERS - 2, 0), ITERS):
        pltpu.make_async_copy(stages[k % 2], out_hbm.at[k], out_sem.at[k % 2]).wait()


def shards(n, excitation, near_tiles, near_offset, near_count, far_src, far_count, source_factor, target_factor):
    excite, panels = excitation.shape
    leaves, slots, leaf, _ = near_tiles.shape
    far_slots, rank, _ = source_factor.shape
    me = lax.axis_index("panels")
    ints = jnp.int32

    own = jnp.arange(leaves, dtype=ints)[:, None] + leaves + near_offset
    near_idx = jnp.where(jnp.arange(slots, dtype=ints)[None, :] < near_count[:, None], own, 3 * leaves)
    live = jnp.arange(far_slots, dtype=ints)[None, :] < far_count[:, None]
    has = jnp.sum(((far_src == me) & live).astype(ints), axis=1)
    rows = jnp.arange(n, dtype=ints)
    before = jnp.sum(jnp.where(rows[None, :] < rows[:, None], has[None, :], 0), axis=1)
    send_idx = jnp.where(has > 0, before, far_slots)
    my_src = lax.dynamic_index_in_dim(far_src, me, 0, keepdims=False)
    my_live = lax.dynamic_index_in_dim(live, me, 0, keepdims=False)
    recv_idx = jnp.where(my_live, my_src, n)
    idx = jnp.concatenate([near_idx.reshape(-1), send_idx, recv_idx]).astype(ints)
    leaf_field = excitation.reshape(excite, leaves, leaf).transpose(1, 0, 2)

    bf, f32 = jnp.bfloat16, jnp.float32
    groups = 4 if leaves % 4 == 0 else 1
    hbm = pl.BlockSpec(memory_space=pl.ANY)
    return pl.pallas_call(
        functools.partial(kernel, n),
        out_shape=jax.ShapeDtypeStruct((ITERS, excite, panels), f32),
        in_specs=[pl.BlockSpec(memory_space=pltpu.SMEM)] + [hbm] * 5,
        out_specs=hbm,
        scratch_shapes=[
            pltpu.VMEM((leaves * slots, leaf, leaf), bf),
            pltpu.VMEM((far_slots * rank, panels), bf),
            pltpu.VMEM((far_slots * rank, panels), bf),
            pltpu.VMEM((excite, panels), bf),
            pltpu.VMEM((3 * leaves + 1, excite, leaf), bf),
            pltpu.VMEM((3 * leaves + 1, excite, leaf), bf),
            pltpu.VMEM((n + 1, rank // 2, 2 * excite), bf),
            pltpu.VMEM((n + 1, rank // 2, 2 * excite), bf),
            pltpu.VMEM((n, rank // 2, 2 * excite), bf),
            pltpu.VMEM((n, rank // 2, 2 * excite), bf),
            pltpu.VMEM((far_slots + 1, rank // 2, 2 * excite), bf),
            pltpu.VMEM((far_slots * rank, excite), f32),
            pltpu.VMEM((excite, panels), f32),
            pltpu.VMEM((excite, panels), f32),
            pltpu.SemaphoreType.DMA((5,)),
            pltpu.SemaphoreType.DMA((2,)),
            pltpu.SemaphoreType.DMA((2, 2, groups)),
            pltpu.SemaphoreType.DMA((2, 2, groups)),
            pltpu.SemaphoreType.DMA((2, n)),
            pltpu.SemaphoreType.DMA((2, n)),
        ],
        compiler_params=pltpu.CompilerParams(
            collective_id=0, has_side_effects=True, vmem_limit_bytes=60 * 1024 * 1024
        ),
    )(
        idx,
        excitation,
        leaf_field,
        near_tiles.reshape(leaves * slots, leaf, leaf),
        source_factor.reshape(far_slots * rank, panels),
        target_factor.reshape(far_slots * rank, panels),
    )


def solution(mesh):
    in_specs = (
        P(None, "panels"),
        P("panels", None, None, None),
        P("panels", None),
        P("panels"),
        P(),
        P(),
        P(None, None, "panels"),
        P(None, None, "panels"),
    )
    return jax.shard_map(
        functools.partial(shards, mesh.shape["panels"]),
        mesh=mesh,
        in_specs=in_specs,
        out_specs=P(None, None, "panels"),
        check_vma=False,
    )
```
